32 devices in a mesh: group: 4 (over y, x), tm: 8 (over z, core).
Axes of the slice: x: 2, y: 2, z: 4, core: 2. Of those that a mesh axis runs over, the one named last changes fastest.
Arguments:
- precip: bfloat16 [4, 32, 1440, 720], P('group', 'tm'), may hold values from 0.099609375 to 4
- day_bins: int32 [32], replicated, may hold values from 0 to 15
- family_of: int32 [4], replicated, may hold values from 0 to 2
Outputs:
- day_mean: bfloat16 [4, 16, 1440, 720], P('group', None, 'tm')
- day_second: bfloat16 [4, 16, 1440, 720], P('group', None, 'tm')
- day_third: bfloat16 [4, 16, 1440, 720], P('group', None, 'tm')
- family_mean: bfloat16 [3, 16, 1440, 720], P(None, None, 'tm')
- anomaly_norm: float32 [4, 32], replicated
The draws below stay inside these ranges and needn't reach their ends.
All inputs are finite; a program needn't handle non-finite values.
Results may differ from the reference program's by a relative error of at most 0.001.
The reference program's roundings to bfloat16 on the way count: a program that leaves them out, or rounds other values in their place, can miss the bound.
Values may be sent and summed in bfloat16 or wider, within the bound.
A program may use at most 192 MiB of HBM per device.

```python
import math
import jax
import jax.numpy as jnp
from jax import lax

LON = 1440
LAT = 720
DAYS = 16
FAM = 3
MODELS = 4
TIME = 32


def with_ends(entries, stream_key, least, top_value):
    longest = entries.shape.index(max(entries.shape))
    spots = []
    for shift in (0, 1):
        where = [jax.random.randint(jax.random.fold_in(stream_key, axis), (), 0, length) for axis, length in enumerate(entries.shape)]
        where[longest] = (where[longest] + shift) % entries.shape[longest]
        spots.append(tuple(where))
    return entries.at[spots[0]].set(least).at[spots[1]].set(top_value)


def block_scale(rng, dims, split, smallest, largest):
    def one(axis_at, parts):
        heights = jax.random.uniform(jax.random.fold_in(jax.random.fold_in(rng, 6), axis_at), (parts,), jnp.float32, smallest / len(split), largest / len(split))
        return jnp.repeat(jnp.exp(heights), dims[axis_at] // parts).reshape((-1,) + (1,) * (len(dims) - axis_at - 1))

    factor_of = one(*split[0])
    for cut in split[1:]:
        factor_of = factor_of * one(*cut)
    return factor_of


def setup_inputs(seed: int = 0) -> dict:
    seeds = jax.random.split(jax.random.key(seed), 4)
    return {
        "precip": jnp.clip(jnp.exp(math.log(4.0) - 3.6927934 * jax.random.uniform(seeds[0], (MODELS, TIME, LON, LAT), jnp.float32) ** block_scale(seeds[0], (MODELS, TIME, LON, LAT), ((0, 4), (1, 8)), -0.2, 0.2)), 0.099609375, 4.0).astype(jnp.bfloat16),
        "day_bins": with_ends(jax.random.randint(seeds[1], (TIME,), 0, DAYS), jax.random.fold_in(seeds[1], 1), 0, DAYS - 1).astype(jnp.int32),
        "family_of": with_ends(jax.random.randint(seeds[2], (MODELS,), 0, FAM), jax.random.fold_in(seeds[2], 1), 0, FAM - 1).astype(jnp.int32),
    }


def lat_weight():
    rows_idx = jnp.arange(LAT, dtype=jnp.float32)
    return jnp.cos((-90.0 + (rows_idx + 0.5) * 180.0 / LAT) * (math.pi / 180.0))

def reference(precip, day_bins, family_of):
    onehot = day_bins[None, :] == jnp.arange(DAYS, dtype=jnp.int32)[:, None]
    onehot_f = onehot.astype(jnp.float32)
    divisor = jnp.maximum(lax.optimization_barrier(jnp.sum(onehot_f, axis=1)), 1.0)
    weight = lat_weight()
    total_weight = LON * jnp.sum(weight)

    def one_model(fields):
        flat_cells = fields.reshape(TIME, LON * LAT)
        bin_sums = jnp.dot(onehot.astype(jnp.bfloat16), flat_cells, preferred_element_type=jnp.float32)
        means = bin_sums / divisor[:, None]
        anomaly = flat_cells.astype(jnp.float32) - jnp.take(means, day_bins, axis=0)
        square = anomaly * anomaly
        second = jnp.dot(onehot_f, square, precision=lax.Precision.HIGHEST) / divisor[:, None]
        third = jnp.dot(onehot_f, square * anomaly, precision=lax.Precision.HIGHEST) / divisor[:, None]
        weighted = lax.optimization_barrier(jnp.sum(square.reshape(TIME, LON, LAT) * weight[None, None, :], axis=(1, 2)))
        norm_value = jnp.sqrt(weighted / total_weight)
        shape = (DAYS, LON, LAT)
        return (means.astype(jnp.bfloat16).reshape(shape), second.astype(jnp.bfloat16).reshape(shape), third.astype(jnp.bfloat16).reshape(shape), norm_value)
    day_mean, day_second, day_third, anomaly_norm = lax.map(one_model, precip)
    family_hot = (family_of[None, :] == jnp.arange(FAM, dtype=jnp.int32)[:, None]).astype(jnp.float32)
    family_count = jnp.maximum(lax.optimization_barrier(jnp.sum(family_hot, axis=1)), 1.0)
    summed = jnp.tensordot(family_hot, day_mean.astype(jnp.float32), axes=1, precision=lax.Precision.HIGHEST)
    family_mean = (summed / family_count[:, None, None, None]).astype(jnp.bfloat16)
    return (day_mean, day_second, day_third, family_mean, anomaly_norm)
```

```python
import functools
import math

import jax
import jax.numpy as jnp
from jax import lax
from jax.experimental import pallas as pl
from jax.experimental.pallas import tpu as pltpu
from jax.sharding import PartitionSpec as P

DAYS = 16
FAM = 3
UNIT = 8
CHUNK = 16
WINDOW = 2
MESH = pl.DeviceIdType.MESH
F32 = jnp.float32
BF16 = jnp.bfloat16


def lat_weight(count):
    rows_idx = jnp.arange(count, dtype=F32)
    return jnp.cos((-90.0 + (rows_idx + 0.5) * 180.0 / count) * (math.pi / 180.0))


def partner(index, k, count):
    if count & (count - 1) == 0:
        return lax.bitwise_xor(index, k)
    return lax.rem(index + k, count)


def sender(index, k, count):
    if count & (count - 1) == 0:
        return lax.bitwise_xor(index, k)
    return lax.rem(index + count - k, count)


def lane_tiles(lats):
    return [(low, min(128, lats - low)) for low in range(0, lats, 128)]


def fused_kernel(
    parts, groups, band, lons, chunks,
    bins, prev, last, inverse, hot, scale, weight, x_ref,
    mean_ref, second_ref, third_ref, family_ref, norm_ref,
    land, slots, run, run2, run3, center, square, nvec, nland, gland,
    own_sem, z_send, z_recv, m_send, m_recv, n_send, n_recv, g_send, g_recv,
):
    steps, span, lats = land.shape
    own = steps // parts
    me, group = lax.axis_index("tm"), lax.axis_index("group")
    relay = groups == 4
    links = (1, 2) if relay else tuple(range(1, groups))
    tiles = lane_tiles(lats)

    barrier = pltpu.get_barrier_semaphore()
    for k in range(1, parts):
        pl.semaphore_signal(barrier, 1, device_id={"tm": partner(me, k, parts)}, device_id_type=MESH)
    for k in range(1, groups):
        pl.semaphore_signal(barrier, 1, device_id={"group": partner(group, k, groups)}, device_id_type=MESH)
    pl.semaphore_wait(barrier, parts + groups - 2)

    def first_row(part):
        low = jnp.minimum(part * band // UNIT * UNIT, lons - span)
        return pl.multiple_of(low, UNIT)

    def z_copy(c, start, rows, k):
        to = partner(me, k, parts)
        return pltpu.make_async_remote_copy(
            src_ref=x_ref.at[:, pl.ds(pl.multiple_of(first_row(to) + start, UNIT), rows)],
            dst_ref=land.at[pl.ds(me * own, own), pl.ds(start, rows)],
            send_sem=z_send.at[c, k - 1],
            recv_sem=z_recv.at[c, k - 1],
            device_id={"tm": to},
            device_id_type=MESH,
        )

    def z_start(c, start, rows):
        for k in range(1, parts):
            z_copy(c, start, rows, k).start()

    own_copy = pltpu.make_async_copy(
        x_ref.at[:, pl.ds(first_row(me), span)], land.at[pl.ds(me * own, own)], own_sem.at[0]
    )
    for c in range(min(WINDOW, len(chunks))):
        z_start(c, *chunks[c])
    own_copy.start()

    zeros = jnp.zeros((UNIT, lats), F32)
    run[steps] = zeros
    run2[steps] = zeros
    run3[steps] = zeros
    square[...] = jnp.zeros_like(square)
    offset = me * band - first_row(me)

    def spread(values, base, out):
        for low, width in tiles:
            part = values[:, :, low : low + width]
            out[pl.ds(base, UNIT), :, low : low + width] = jnp.swapaxes(part, 0, 1).astype(BF16)

    def unit(base):
        def add(t, carry):
            x = land[t, pl.ds(base, UNIT), :].astype(F32)
            run[t] = run[prev[t]] + x
            return carry

        lax.fori_loop(0, steps, add, 0, unroll=4)

        def mean(b, carry):
            center[b] = run[last[b]] * inverse[b]
            return carry

        lax.fori_loop(0, DAYS, mean, 0, unroll=2)
        spread(center, base, mean_ref)
        row = lax.broadcasted_iota(jnp.int32, (UNIT, lats), 0) + base - offset
        valid = jnp.logical_and(row >= 0, row < band)

        def moment(t, carry):
            a = land[t, pl.ds(base, UNIT), :].astype(F32) - center[bins[t]]
            q = a * a
            run2[t] = run2[prev[t]] + q
            run3[t] = run3[prev[t]] + q * a
            square[t] += jnp.where(valid, q, 0.0)
            return carry

        lax.fori_loop(0, steps, moment, 0, unroll=4)
        for source, out in ((run2, second_ref), (run3, third_ref)):
            def close(b, carry, source=source):
                center[b] = source[last[b]] * inverse[b]
                return carry

            lax.fori_loop(0, DAYS, close, 0, unroll=2)
            spread(center, base, out)

    def m_copy(c, start, rows, way):
        half = rows // 2
        if way < len(links):
            k, slot = links[way], links[way] - 1
            source, low, count = mean_ref, start, rows
        elif way == 2:
            k, slot, low, count = 2, 2, start, half
            source = slots.at[0]
        else:
            k, slot, low, count = 1, 2, start + half, rows - half
            source = slots.at[1]
        return pltpu.make_async_remote_copy(
            src_ref=source.at[pl.ds(low, count)],
            dst_ref=slots.at[slot, pl.ds(low, count)],
            send_sem=m_send.at[c, way],
            recv_sem=m_recv.at[c, way],
            device_id={"group": partner(group, k, groups)},
            device_id_type=MESH,
        )

    def family(start, rows):
        owner = [group] + [sender(group, k, groups) for k in range(1, groups)]
        factor = [[hot[f, owner[k]] for k in range(groups)] for f in range(FAM)]

        def one(r, carry):
            at = start + r
            fields = [mean_ref[at].astype(F32)] + [slots[k, at].astype(F32) for k in range(groups - 1)]
            for f in range(FAM):
                total = fields[0] * factor[f][0]
                for k in range(1, groups):
                    total = total + fields[k] * factor[f][k]
                family_ref[f, at] = (total * scale[f]).astype(BF16)
            return carry

        lax.fori_loop(0, rows, one, 0)

    def arrive(c, start, rows):
        for k in range(1, parts):
            z_copy(c, start, rows, k).wait_recv()

    def compute(start, rows):
        lax.fori_loop(
            0, rows // UNIT, lambda u, carry: (unit(pl.multiple_of(start + u * UNIT, UNIT)), carry)[1], 0
        )

    def share(c, start, rows):
        for way in range(len(links)):
            m_copy(c, start, rows, way).start()

    def pass_on(c, start, rows):
        for way in range(len(links)):
            m_copy(c, start, rows, way).wait_recv()
        if relay:
            m_copy(c, start, rows, 2).start()
            m_copy(c, start, rows, 3).start()

    def finish(c, start, rows):
        if relay:
            m_copy(c, start, rows, 2).wait_recv()
            m_copy(c, start, rows, 3).wait_recv()
        family(start, rows)

    count = len(chunks)
    even = sum(rows == CHUNK for _, rows in chunks)

    def step(s):
        if s < count:
            arrive(s, *chunks[s])
            if s + WINDOW < count:
                z_start(s + WINDOW, *chunks[s + WINDOW])
            if s == 0:
                own_copy.wait()
            compute(*chunks[s])
            share(s, *chunks[s])
        if 0 < s <= count:
            pass_on(s - 1, *chunks[s - 1])
        if s >= 2:
            finish(s - 2, *chunks[s - 2])

    def middle(s, carry):
        at = lambda c: (c, pl.multiple_of(c * CHUNK, CHUNK), CHUNK)
        arrive(*at(s))
        z_start(*at(s + WINDOW))
        compute(*at(s)[1:])
        share(*at(s))
        pass_on(*at(s - 1))
        finish(*at(s - 2))
        return carry

    high = max(2, even - WINDOW)
    for s in range(min(2, count)):
        step(s)
    lax.fori_loop(2, high, middle, 0)
    for s in range(high, count):
        step(s)

    lanes = nvec.shape[-1]
    folded = jnp.sum(square[...], axis=1) * weight[...]
    totals = jnp.sum(folded, axis=1, keepdims=True)
    here = lax.broadcasted_iota(jnp.int32, (steps, lanes), 0) == lax.broadcasted_iota(
        jnp.int32, (steps, lanes), 1
    )
    mine = jnp.sum(jnp.where(here, totals, 0.0), axis=0, keepdims=True)
    nvec[0] = mine
    nland[me] = mine

    def n_copy(k):
        return pltpu.make_async_remote_copy(
            src_ref=nvec.at[0], dst_ref=nland.at[me], send_sem=n_send.at[k - 1], recv_sem=n_recv.at[k - 1],
            device_id={"tm": partner(me, k, parts)}, device_id_type=MESH,
        )

    def g_copy(k):
        return pltpu.make_async_remote_copy(
            src_ref=nvec.at[1], dst_ref=gland.at[group], send_sem=g_send.at[k - 1], recv_sem=g_recv.at[k - 1],
            device_id={"group": partner(group, k, groups)}, device_id_type=MESH,
        )

    for k in range(1, parts):
        n_copy(k).start()
    step(count)
    for k in range(1, parts):
        n_copy(k).wait_recv()
    model = nland[0]
    for k in range(1, parts):
        model = model + nland[k]
    nvec[1] = model
    gland[group] = model
    for k in range(1, groups):
        g_copy(k).start()
    step(count + 1)
    for k in range(1, groups):
        g_copy(k).wait_recv()
    norm_ref[...] = gland[...]

    for k in range(1, parts):
        n_copy(k).wait_send()
    for k in range(1, groups):
        g_copy(k).wait_send()
    for c in range(count):
        for k in range(1, parts):
            z_copy(c, *chunks[c], k).wait_send()
        for way in range(len(links) + (2 if relay else 0)):
            m_copy(c, *chunks[c], way).wait_send()


def fused(x, scalars, weight, parts, groups, band, span, chunks):
    own, lons, lats = x.shape
    steps = own * parts
    lanes = -(-steps // 128) * 128
    smem = pl.BlockSpec(memory_space=pltpu.SMEM)
    vmem = pl.BlockSpec(memory_space=pltpu.VMEM)
    ways = 4 if groups == 4 else groups - 1
    dma = pltpu.SemaphoreType.DMA
    wide = -(-lats // 128) * 128
    scratch = [
        ((steps, span, lats), BF16),
        ((groups - 1, span, DAYS, lats), BF16),
        ((steps + 1, UNIT, lats), F32),
        ((steps + 1, UNIT, lats), F32),
        ((steps + 1, UNIT, lats), F32),
        ((DAYS, UNIT, lats), F32),
        ((steps, UNIT, lats), F32),
        ((2, 1, lanes), F32),
        ((parts, 1, lanes), F32),
        ((groups, 1, lanes), F32),
    ]
    size = sum(math.prod(shape[:-1]) * wide * jnp.dtype(kind).itemsize for shape, kind in scratch)
    field = pltpu.VMEM((span, DAYS, lats), BF16)
    return pl.pallas_call(
        functools.partial(fused_kernel, parts, groups, band, lons, chunks),
        in_specs=[smem] * 6 + [vmem, pl.BlockSpec(memory_space=pl.ANY)],
        out_specs=[vmem] * 5,
        out_shape=[field] * 3
        + [pltpu.VMEM((FAM, span, DAYS, lats), BF16), pltpu.VMEM((groups, 1, lanes), F32)],
        scratch_shapes=[pltpu.VMEM(shape, kind) for shape, kind in scratch]
        + [
            dma((1,)),
            dma((len(chunks), parts - 1)),
            dma((len(chunks), parts - 1)),
            dma((len(chunks), ways)),
            dma((len(chunks), ways)),
            dma((parts - 1,)),
            dma((parts - 1,)),
            dma((groups - 1,)),
            dma((groups - 1,)),
        ],
        compiler_params=pltpu.CompilerParams(
            collective_id=0, has_side_effects=True, vmem_limit_bytes=size + 3 * 2**20
        ),
        cost_estimate=pl.CostEstimate(
            flops=20 * steps * span * lats, bytes_accessed=8 * steps * span * lats, transcendentals=0
        ),
    )(*scalars, weight, x)


def place_kernel(steps, offset, total, mean, second, third, family, norm, *refs):
    outs, norm_out, sem = refs[:4], refs[4], refs[5]
    rows = outs[0].shape[0]
    copies = [
        pltpu.make_async_copy(a.at[pl.ds(offset[0], rows)], o, sem.at[i])
        for i, (a, o) in enumerate(zip((mean, second, third), outs))
    ]
    copies += [
        pltpu.make_async_copy(family.at[f, pl.ds(offset[0], rows)], outs[3].at[f], sem.at[3 + f])
        for f in range(family.shape[0])
    ]
    for copy in copies:
        copy.start()
    for g in range(norm.shape[0]):
        norm_out[pl.ds(g, 1), :] = jnp.sqrt(norm[g][:, :steps] / total[0])
    for copy in copies:
        copy.wait()


def place(fields, offset, total, steps, band):
    mean, norm = fields[0], fields[4]
    _, days, lats = mean.shape
    smem = pl.BlockSpec(memory_space=pltpu.SMEM)
    hbm = pl.BlockSpec(memory_space=pl.ANY)
    vmem = pl.BlockSpec(memory_space=pltpu.VMEM)
    out = jax.ShapeDtypeStruct((band, days, lats), BF16)
    return pl.pallas_call(
        functools.partial(place_kernel, steps),
        in_specs=[smem, smem] + [vmem] * 5,
        out_specs=[hbm] * 4 + [vmem],
        out_shape=[out] * 3
        + [
            jax.ShapeDtypeStruct((FAM, band, days, lats), BF16),
            jax.ShapeDtypeStruct((norm.shape[0], steps), F32),
        ],
        scratch_shapes=[pltpu.SemaphoreType.DMA((3 + FAM,))],
        compiler_params=pltpu.CompilerParams(vmem_limit_bytes=2**20),
    )(offset, total, *fields)


def local(parts, groups, precip, day_bins, family_of):
    _, own, lons, lats = precip.shape
    band = lons // parts
    steps = own * parts
    span = -(-(band + max(p * band % UNIT for p in range(parts))) // UNIT) * UNIT
    whole = (span - UNIT) // CHUNK
    chunks = [(c * CHUNK, CHUNK) for c in range(whole)]
    chunks += [(low, UNIT) for low in range(whole * CHUNK, span, UNIT)]

    time = jnp.arange(steps, dtype=jnp.int32)
    days = jnp.arange(DAYS, dtype=jnp.int32)
    onehot = day_bins[None, :] == days[:, None]
    inverse = 1.0 / jnp.maximum(jnp.sum(onehot.astype(F32), axis=1), 1.0)
    last = jnp.max(jnp.where(onehot, time[None, :], -1), axis=1)
    last = jnp.where(last < 0, steps, last)
    before = (day_bins[None, :] == day_bins[:, None]) & (time[None, :] < time[:, None])
    prev = jnp.max(jnp.where(before, time[None, :], -1), axis=1)
    prev = jnp.where(prev < 0, steps, prev)
    hot = (family_of[None, :] == jnp.arange(FAM, dtype=jnp.int32)[:, None]).astype(F32)
    scale = 1.0 / jnp.maximum(jnp.sum(hot, axis=1), 1.0)
    weight = lat_weight(lats)
    total = (lons * jnp.sum(weight)).reshape(1)

    scalars = (day_bins, prev, last, inverse, hot, scale)
    fields = fused(precip[0], scalars, weight[None, :], parts, groups, band, span, chunks)
    me = lax.axis_index("tm")
    offset = (me * band - jnp.minimum(me * band // UNIT * UNIT, lons - span)).reshape(1).astype(jnp.int32)
    mean, second, third, family, norm = place(fields, offset, total, steps, band)
    turned = [jnp.swapaxes(a, 0, 1)[None] for a in (mean, second, third)]
    return (*turned, jnp.swapaxes(family, 1, 2), norm)


def solution(mesh):
    in_specs = (P("group", "tm", None, None), P(), P())
    out_specs = (
        P("group", None, "tm", None),
        P("group", None, "tm", None),
        P("group", None, "tm", None),
        P(None, None, "tm", None),
        P(),
    )
    body = functools.partial(local, mesh.shape["tm"], mesh.shape["group"])
    return jax.shard_map(body, mesh=mesh, in_specs=in_specs, out_specs=out_specs, check_vma=False)
```
